32 devices in a mesh: section: 4 (over y, core), tensor: 2 (over x), dp: 4 (over z).
Axes of the slice: x: 2, y: 2, z: 4, core: 2. Of those that a mesh axis runs over, the one named last changes fastest.
Arguments:
- acts: bfloat16 [4, 8, 256, 2048], P('section', 'dp', 'tensor'), parts along dimension 1, may hold values from -6 to 6
- fresh: bfloat16 [8, 256, 2048], P('dp', 'tensor'), parts along dimension 0, may hold values from -6 to 6
- order: int32 [4, 2], P('section'), may hold values from 0 to 1
- ln_gain: float32 [4, 2048], P('section'), may hold values from 0.1 to 1.9
- ln_bias: float32 [4, 2048], P('section'), may hold values from -3 to 3
- wqkv: bfloat16 [4, 2048, 6144], P('section', None, 'tensor'), may hold values from -4 to 4
- wo: bfloat16 [4, 2048, 2048], P('section', 'tensor'), may hold values from -0.125 to 0.125
Outputs:
- section_out: bfloat16 [8, 4, 256, 2048], P('dp', 'section', 'tensor'), parts along dimension 0
- held: bfloat16 [4, 8, 256, 2048], P('section', 'dp', 'tensor'), parts along dimension 1
The draws below stay inside these ranges and needn't reach their ends.
There are 4 independent parts, one for each index of `dp`. The reference program is written for one: setup_inputs(seed, part) draws one part's arguments, and reference() takes and returns one part's arrays. A program takes and returns all parts, laid end to end along the dimension named above; an argument that names none is the same for every part. Nothing has to cross between parts.
All inputs are finite; a program needn't handle non-finite values.
Results may differ from the reference program's by a relative error of at most 0.017.
Values may be sent and summed in bfloat16 or wider, within the bound.
A program may use at most 64 MiB of HBM per device.

```python
import jax
import jax.numpy as jnp
from jax import lax

D = 2048
HEADS = 16
HD = 128
SEQ = 256
SLOTS = 2
TICKS = 2
SECTIONS = 4
N_TENSOR = 2


def draw_wqkv(key, part):
    first = jax.random.fold_in(jax.random.fold_in(key, 11), 0)
    base = jnp.clip(jax.random.normal(first, (SECTIONS, D, HEADS, 3, HD), jnp.float32), -6.0, 6.0) * D ** (-0.5)
    return base.reshape(SECTIONS, D, HEADS * 3 * HD).astype(jnp.bfloat16)


def with_ends(values, own_key, smallest, largest):
    longest = values.shape.index(max(values.shape))
    spots = []
    for shift in (0, 1):
        where = [jax.random.randint(jax.random.fold_in(own_key, axis), (), 0, length) for axis, length in enumerate(values.shape)]
        where[longest] = (where[longest] + shift) % values.shape[longest]
        spots.append(tuple(where))
    return values.at[spots[0]].set(smallest).at[spots[1]].set(largest)


def level_of(rng, shape, cuts, low, high):
    loudness = 1.0
    for axis_at, blocks in cuts:
        steps = jax.random.uniform(jax.random.fold_in(jax.random.fold_in(rng, 6), axis_at), (blocks,), jnp.float32, low / len(cuts), high / len(cuts))
        loudness = loudness * jnp.repeat(jnp.exp(steps), shape[axis_at] // blocks).reshape((-1,) + (1,) * (len(shape) - 1 - axis_at))
    return loudness


def normal_values(rng, shape, scale, limit, cuts=(), kind=jnp.bfloat16):
    entries = jax.random.normal(rng, shape, jnp.float32) * scale
    if len(cuts) > 0:
        entries = level_of(rng, shape, cuts, -0.22, 0.18) * entries
    return jnp.clip(entries, min=-limit, max=limit).astype(kind)


def setup_inputs(seed: int = 0, part: int = 0) -> dict:
    key_list = jax.random.split(jax.random.key(seed), 8)
    own_keys = jax.random.split(jax.random.fold_in(key_list[7], part), 8)
    acts = normal_values(own_keys[0], (SECTIONS, SLOTS, SEQ, D), 1.0, 6.0, ((0, 4), (2, 2)))
    fresh = normal_values(own_keys[1], (TICKS, SEQ, D), 1.0, 6.0, ((1, 2),))
    order = with_ends(jax.random.randint(key_list[2], (SECTIONS, TICKS), 0, SLOTS), jax.random.fold_in(key_list[2], 1), 0, SLOTS - 1).astype(jnp.int32)
    ln_gain = jnp.clip(1.0 + 0.18 * jax.random.normal(key_list[3], (SECTIONS, D), jnp.float32), 0.1, 1.9)
    ln_bias = normal_values(key_list[4], (SECTIONS, D), 0.5, 3.0, ((0, 4),), jnp.float32)
    wqkv = draw_wqkv(jax.random.fold_in(key_list[7], 71), part)
    wo = normal_values(key_list[6], (SECTIONS, HEADS * HD, D), (HEADS * HD) ** -0.5, 0.125, ((0, 4), (1, 2)))
    return {"acts": acts, "fresh": fresh, "order": order, "ln_gain": ln_gain, "ln_bias": ln_bias, "wqkv": wqkv, "wo": wo}


def normed(rows, gain, bias):
    values = rows.astype(jnp.float32)
    centred = values - lax.optimization_barrier(jnp.mean(values, axis=-1, keepdims=True))
    spread = lax.optimization_barrier(jnp.mean(centred * centred, axis=-1, keepdims=True))
    return (centred * lax.rsqrt(spread + 1e-06) * gain + bias).astype(jnp.bfloat16)

def layer(inputs):
    rows, gain, bias, w_in, w_out = inputs
    normal_rows = normed(rows, gain, bias)
    qkv = jnp.dot(normal_rows, w_in, preferred_element_type=jnp.float32).astype(jnp.bfloat16)
    grid = qkv.reshape(SEQ, HEADS, 3, HD).astype(jnp.float32)
    scores = jnp.einsum('qhe,khe->hqk', grid[:, :, 0], grid[:, :, 1]) / jnp.sqrt(jnp.float32(HD))
    probs = jax.nn.softmax(scores, axis=-1).astype(jnp.bfloat16)
    attn = jnp.einsum('hqk,khe->qhe', probs.astype(jnp.float32), grid[:, :, 2]).astype(jnp.bfloat16)
    grouped = attn.reshape(SEQ, N_TENSOR, HEADS // N_TENSOR * HD).astype(jnp.float32)
    wo_grouped = w_out.reshape(N_TENSOR, HEADS // N_TENSOR * HD, D).astype(jnp.float32)
    partial_value = jnp.einsum('sgc,gcd->gsd', grouped, wo_grouped).astype(jnp.bfloat16)
    partial_value = lax.optimization_barrier(partial_value)
    total = lax.optimization_barrier(jnp.sum(partial_value.astype(jnp.float32), axis=0))
    return (rows.astype(jnp.float32) + total).astype(jnp.bfloat16)

def reference(acts, fresh, order, ln_gain, ln_bias, wqkv, wo):
    slots = acts
    outputs = []
    slot_ids = jnp.arange(SLOTS, dtype=jnp.int32)
    for tick in range(TICKS):
        chosen = order[:, tick].astype(jnp.int32)
        picked = jnp.take_along_axis(slots, chosen[:, None, None, None], axis=1)[:, 0]
        results = lax.map(layer, (picked, ln_gain, ln_bias, wqkv, wo))
        outputs.append(results)
        incoming = jnp.concatenate([fresh[tick][None], results[:-1]], axis=0)
        marks = (slot_ids[None, :] == chosen[:, None])[:, :, None, None]
        slots = jnp.where(marks, incoming[:, None], slots)
    return (jnp.stack(outputs, axis=0), slots)
```

```python
import functools
import math

import jax
import jax.numpy as jnp
from jax import lax
from jax.experimental import pallas as pl
from jax.experimental.pallas import tpu as pltpu
from jax.sharding import PartitionSpec as P

HD = 128
EPS = 1e-06
CHUNK = 32
BLOCK = 64
TILE = 512
PIECE = 16
MESH = pl.DeviceIdType.MESH


def relay(
    acts, fresh, order, gain, bias, w_in, w_out, out, held,
    slots, fresh_v, wi, wo, xs, h, qkv, mixed, part, got, res, arr,
    load_sem, wi_sem, wo_sem, out_sem, held_sem,
    ag_send, ag_recv, rs_send, rs_recv, hop_send, hop_recv,
):
    ticks, rows, width = fresh.shape
    n_slots = acts.shape[1]
    peers = lax.axis_size("tensor")
    sections = lax.axis_size("section")
    me = lax.axis_index("tensor")
    sec = lax.axis_index("section")
    seq = rows * peers
    heads = wi.shape[1] // (3 * HD)
    block = min(BLOCK, rows)
    chunk = min(CHUNK, block)
    n_chunks = rows // chunk
    n_blocks = rows // block
    per_block = block // chunk
    wi_tile = min(TILE, wi.shape[1])
    wo_tile = min(TILE, width)
    has_prev = sec > 0
    has_next = sec < sections - 1

    load_acts = pltpu.make_async_copy(acts.at[0], slots, load_sem.at[0])
    load_acts.start()

    def wi_copy(i):
        cols = pl.ds(pl.multiple_of(i * wi_tile, wi_tile), wi_tile)
        return pltpu.make_async_copy(w_in.at[0, :, cols], wi.at[:, cols], wi_sem.at[i])

    for i in range(wi.shape[1] // wi_tile):
        wi_copy(i).start()
    load_wo = pltpu.make_async_copy(w_out.at[0], wo, wo_sem)
    load_wo.start()
    load_fresh = pltpu.make_async_copy(fresh, fresh_v, load_sem.at[1])
    load_fresh.start()

    barrier = pltpu.get_barrier_semaphore()
    for d in range(1, peers):
        pl.semaphore_signal(
            barrier, inc=1, device_id={"tensor": lax.rem(me + d, peers)}, device_id_type=MESH
        )

    @pl.when(has_prev)
    def _():
        pl.semaphore_signal(barrier, inc=1, device_id={"section": sec - 1}, device_id_type=MESH)

    @pl.when(has_next)
    def _():
        pl.semaphore_signal(barrier, inc=1, device_id={"section": sec + 1}, device_id_type=MESH)

    def ag_copy(t, d, c):
        return pltpu.make_async_remote_copy(
            src_ref=xs.at[t, 0, pl.ds(c * chunk, chunk)],
            dst_ref=xs.at[t, d, pl.ds(c * chunk, chunk)],
            send_sem=ag_send.at[t, d - 1, c],
            recv_sem=ag_recv.at[t, d - 1, c],
            device_id={"tensor": lax.rem(me + d, peers)},
            device_id_type=MESH,
        )

    def rs_copy(t, d, c):
        return pltpu.make_async_remote_copy(
            src_ref=part.at[t, d, pl.ds(c * chunk, chunk)],
            dst_ref=got.at[t, d - 1, pl.ds(c * chunk, chunk)],
            send_sem=rs_send.at[t, d - 1, c],
            recv_sem=rs_recv.at[t, d - 1, c],
            device_id={"tensor": lax.rem(me - d + peers, peers)},
            device_id_type=MESH,
        )

    def hop_copy(t, c):
        return pltpu.make_async_remote_copy(
            src_ref=res.at[t, pl.ds(c * chunk, chunk)],
            dst_ref=arr.at[t, pl.ds(c * chunk, chunk)],
            send_sem=hop_send.at[t, c],
            recv_sem=hop_recv.at[t, c],
            device_id={"section": lax.rem(sec + 1, sections)},
            device_id_type=MESH,
        )

    def pieces(start, count, step):
        def one(i, carry):
            step(pl.ds(pl.multiple_of(start + i * PIECE, PIECE), PIECE))
            return carry

        lax.fori_loop(0, count // PIECE, one, 0)

    def offer(t, c):
        chosen = order[0, t]

        def step(r):
            xs[t, 0, r, :] = slots[chosen, r, :]

        pieces(c * chunk, chunk, step)

    def send_offer(t, c):
        for d in range(1, peers):
            ag_copy(t, d, c).start()

    def norm(t, d, start, count):
        g = gain[0:1, :]
        b = bias[0:1, :]

        def step(r):
            values = xs[t, d, r, :].astype(jnp.float32)
            centred = values - jnp.mean(values, axis=-1, keepdims=True)
            spread = jnp.mean(centred * centred, axis=-1, keepdims=True)
            h[r, :] = (centred * lax.rsqrt(spread + EPS) * g + b).astype(jnp.bfloat16)

        pieces(start, count, step)

    def project(d, start, count, first):
        def one(i, carry):
            if first:
                wi_copy(i).wait()
            cols = pl.ds(pl.multiple_of(i * wi_tile, wi_tile), wi_tile)
            y = jnp.dot(h[pl.ds(start, count), :], wi[:, cols], preferred_element_type=jnp.float32)
            qkv[pl.ds(d * rows + start, count), cols] = y.astype(jnp.bfloat16)
            return carry

        lax.fori_loop(0, wi.shape[1] // wi_tile, one, 0)

    scale = math.log2(math.e) / math.sqrt(HD)

    def attend(t, d, b):
        r = pl.ds(pl.multiple_of(d * rows + b * block, block), block)
        for n in range(heads):
            base = n * 3 * HD
            q = qkv[r, base:base + HD]
            k = qkv[:, base + HD:base + 2 * HD]
            v = qkv[:, base + 2 * HD:base + 3 * HD]
            s = lax.dot_general(q, k, (((1,), (1,)), ((), ())), preferred_element_type=jnp.float32)
            e = jnp.exp2((s - jnp.max(s, axis=-1, keepdims=True)) * scale)
            total = jnp.sum(e, axis=-1, keepdims=True)
            y = jnp.dot(e.astype(jnp.bfloat16), v, preferred_element_type=jnp.float32)
            mixed[:, n * HD:(n + 1) * HD] = (y / total).astype(jnp.bfloat16)

        def one(i, carry):
            cols = pl.ds(pl.multiple_of(i * wo_tile, wo_tile), wo_tile)
            y = jnp.dot(mixed[...], wo[:, cols], preferred_element_type=jnp.float32)
            part[t, d, pl.ds(pl.multiple_of(b * block, block), block), cols] = y.astype(jnp.bfloat16)
            return carry

        lax.fori_loop(0, width // wo_tile, one, 0)

    def finish(t, c):
        for d in range(1, peers):
            rs_copy(t, d, c).wait_recv()

        def step(r):
            total = part[t, 0, r, :].astype(jnp.float32)
            for d in range(1, peers):
                total = total + got[t, d - 1, r, :].astype(jnp.float32)
            res[t, r, :] = (xs[t, 0, r, :].astype(jnp.float32) + total).astype(jnp.bfloat16)

        pieces(c * chunk, chunk, step)

        @pl.when(has_next)
        def _():
            hop_copy(t, c).start()

    def take(t, c):
        chosen = order[0, t]

        @pl.when(has_prev)
        def _():
            hop_copy(t, c).wait_recv()

        def step(r, source):
            new = source[t, r, :].astype(jnp.float32)
            for k in range(n_slots):
                old = slots[k, r, :].astype(jnp.float32)
                slots[k, r, :] = jnp.where(chosen == k, new, old).astype(jnp.bfloat16)

        @pl.when(has_prev)
        def _():
            pieces(c * chunk, chunk, functools.partial(step, source=arr))

        @pl.when(jnp.logical_not(has_prev))
        def _():
            pieces(c * chunk, chunk, functools.partial(step, source=fresh_v))

    def held_copy(c):
        r = pl.ds(c * chunk, chunk)
        return pltpu.make_async_copy(slots.at[:, r], held.at[0, :, r], held_sem.at[c])

    def out_copy(t):
        return pltpu.make_async_copy(res.at[t], out.at[t, 0], out_sem.at[t])

    load_acts.wait()
    for c in range(n_chunks):
        offer(0, c)
    pl.semaphore_wait(
        barrier, peers - 1 + has_prev.astype(jnp.int32) + has_next.astype(jnp.int32)
    )
    for c in range(n_chunks):
        send_offer(0, c)

    for t in range(ticks):
        norm(t, 0, 0, rows)
        project(0, 0, rows, t == 0)
        for b in range(n_blocks):
            for d in range(1, peers):
                for c in range(b * per_block, (b + 1) * per_block):
                    ag_copy(t, d, c).wait_recv()
                norm(t, d, b * block, block)
                project(d, b * block, block, False)
        if t == 0:
            load_wo.wait()
        for d in [*range(1, peers), 0]:
            def blocks(b, carry, d=d):
                attend(t, d, b)
                if d:
                    for c in range(per_block):
                        rs_copy(t, d, b * per_block + c).start()
                return carry

            lax.fori_loop(0, n_blocks, blocks, 0)
        if t == 0:
            load_fresh.wait()
        lag = 1
        for step in range(n_chunks + lag):
            if step < n_chunks:
                finish(t, step)
            if step == n_chunks - 1:
                out_copy(t).start()
            if step >= lag:
                take(t, step - lag)
                if t + 1 < ticks:
                    offer(t + 1, step - lag)
                    send_offer(t + 1, step - lag)
                else:
                    held_copy(step - lag).start()

    for t in range(ticks):
        for c in range(n_chunks):
            for d in range(1, peers):
                ag_copy(t, d, c).wait_send()
                rs_copy(t, d, c).wait_send()

            @pl.when(has_next)
            def _():
                hop_copy(t, c).wait_send()

        out_copy(t).wait()
    for c in range(n_chunks):
        held_copy(c).wait()


def body(acts, fresh, order, ln_gain, ln_bias, wqkv, wo):
    ticks, rows, width = fresh.shape
    n_slots = acts.shape[1]
    peers = lax.axis_size("tensor")
    seq = rows * peers
    block = min(BLOCK, rows)
    n_chunks = rows // min(CHUNK, block)
    inner = wo.shape[1]
    wide = wqkv.shape[2]
    bf = jnp.bfloat16
    dma = pltpu.SemaphoreType.DMA
    anywhere = pl.BlockSpec(memory_space=pl.ANY)
    vmem = pl.BlockSpec(memory_space=pltpu.VMEM)
    smem = pl.BlockSpec(memory_space=pltpu.SMEM)
    return pl.pallas_call(
        relay,
        out_shape=(
            jax.ShapeDtypeStruct((ticks, 1, rows, width), bf),
            jax.ShapeDtypeStruct((1, n_slots, rows, width), bf),
        ),
        in_specs=[anywhere, anywhere, smem, vmem, vmem, anywhere, anywhere],
        out_specs=(anywhere, anywhere),
        scratch_shapes=[
            pltpu.VMEM((n_slots, rows, width), bf),
            pltpu.VMEM((ticks, rows, width), bf),
            pltpu.VMEM((width, wide), bf),
            pltpu.VMEM((inner, width), bf),
            pltpu.VMEM((ticks, peers, rows, width), bf),
            pltpu.VMEM((rows, width), bf),
            pltpu.VMEM((seq, wide), bf),
            pltpu.VMEM((block, inner), bf),
            pltpu.VMEM((ticks, peers, rows, width), bf),
            pltpu.VMEM((ticks, peers - 1, rows, width), bf),
            pltpu.VMEM((ticks, rows, width), bf),
            pltpu.VMEM((ticks, rows, width), bf),
            dma((2,)),
            dma((wide // min(TILE, wide),)),
            dma,
            dma((ticks,)),
            dma((n_chunks,)),
            dma((ticks, peers - 1, n_chunks)),
            dma((ticks, peers - 1, n_chunks)),
            dma((ticks, peers - 1, n_chunks)),
            dma((ticks, peers - 1, n_chunks)),
            dma((ticks, n_chunks)),
            dma((ticks, n_chunks)),
        ],
        compiler_params=pltpu.CompilerParams(
            collective_id=0, has_side_effects=True, vmem_limit_bytes=60 * 1024 * 1024
        ),
    )(acts, fresh, order, ln_gain, ln_bias, wqkv, wo)


def solution(mesh):
    return jax.shard_map(
        body,
        mesh=mesh,
        in_specs=(
            P("section", "dp", "tensor", None),
            P("dp", "tensor", None),
            P("section", None),
            P("section", None),
            P("section", None),
            P("section", None, "tensor"),
            P("section", "tensor", None),
        ),
        out_specs=(P("dp", "section", "tensor", None), P("section", "dp", "tensor", None)),
        check_vma=False,
    )
```

```python
import functools
import math

import jax
import jax.numpy as jnp
from jax import lax
from jax.experimental import pallas as pl
from jax.experimental.pallas import tpu as pltpu
from jax.sharding import PartitionSpec as P

HD = 128
EPS = 1e-06
CHUNK = 512
TILE = 1024
NORM_ROWS = 16
PIECE = 32
MESH = pl.DeviceIdType.MESH


def fitting(most, size):
    return math.gcd(most, size)


def relay(
    acts, fresh, order, gain, bias, w_in, w_out, out, held,
    slots, fresh_v, wi, wo, xs, h, qkv, mixed, part, got, res, arr,
    acts_sem, fresh_sem, wi_sem, wo_sem, out_sem, held_sem,
    ag_send, ag_recv, rs_send, rs_recv, hop_send, hop_recv,
):
    ticks, rows, width = fresh.shape
    n_slots = acts.shape[1]
    peers = lax.axis_size("tensor")
    sections = lax.axis_size("section")
    me = lax.axis_index("tensor")
    sec = lax.axis_index("section")
    seq = rows * peers
    heads = wi.shape[1] // (3 * HD)
    chunk = fitting(CHUNK, width)
    n_chunks = width // chunk
    wi_tile = fitting(TILE, wi.shape[1])
    n_tiles = wi.shape[1] // wi_tile
    has_prev = sec > 0
    has_next = sec < sections - 1

    def span(c):
        return pl.ds(c * chunk, chunk)

    def acts_copy(c):
        return pltpu.make_async_copy(acts.at[0, :, :, span(c)], slots.at[:, :, span(c)], acts_sem.at[c])

    for c in range(n_chunks):
        acts_copy(c).start()

    def wi_copy(i):
        cols = pl.ds(i * wi_tile, wi_tile)
        return pltpu.make_async_copy(w_in.at[0, :, cols], wi.at[:, cols], wi_sem.at[i])

    for i in range(n_tiles):
        wi_copy(i).start()
    load_wo = pltpu.make_async_copy(w_out.at[0], wo, wo_sem)
    load_wo.start()
    load_fresh = pltpu.make_async_copy(fresh, fresh_v, fresh_sem)
    load_fresh.start()

    barrier = pltpu.get_barrier_semaphore()
    for d in range(1, peers):
        pl.semaphore_signal(
            barrier, inc=1, device_id={"tensor": lax.rem(me + d, peers)}, device_id_type=MESH
        )

    @pl.when(has_prev)
    def _():
        pl.semaphore_signal(barrier, inc=1, device_id={"section": sec - 1}, device_id_type=MESH)

    @pl.when(has_next)
    def _():
        pl.semaphore_signal(barrier, inc=1, device_id={"section": sec + 1}, device_id_type=MESH)

    def ag_copy(t, d, c):
        return pltpu.make_async_remote_copy(
            src_ref=xs.at[t, 0, :, span(c)],
            dst_ref=xs.at[t, d, :, span(c)],
            send_sem=ag_send.at[t, d - 1, c],
            recv_sem=ag_recv.at[t, d - 1, c],
            device_id={"tensor": lax.rem(me + d, peers)},
            device_id_type=MESH,
        )

    def rs_copy(t, d, c):
        return pltpu.make_async_remote_copy(
            src_ref=part.at[t, d, :, span(c)],
            dst_ref=got.at[t, d - 1, :, span(c)],
            send_sem=rs_send.at[t, d - 1, c],
            recv_sem=rs_recv.at[t, d - 1, c],
            device_id={"tensor": lax.rem(me - d + peers, peers)},
            device_id_type=MESH,
        )

    def hop_copy(t, c):
        return pltpu.make_async_remote_copy(
            src_ref=res.at[t, :, span(c)],
            dst_ref=arr.at[t, :, span(c)],
            send_sem=hop_send.at[t, c],
            recv_sem=hop_recv.at[t, c],
            device_id={"section": lax.rem(sec + 1, sections)},
            device_id_type=MESH,
        )

    def pieces(step):
        for i in range(rows // PIECE):
            step(pl.ds(i * PIECE, PIECE))

    def offer(t, c):
        chosen = order[0, t]

        def step(r):
            x = slots[0, r, span(c)].astype(jnp.float32)
            for k in range(1, n_slots):
                x = jnp.where(chosen == k, slots[k, r, span(c)].astype(jnp.float32), x)
            xs[t, 0, r, span(c)] = x.astype(jnp.bfloat16)

        pieces(step)

    def send_offer(t, c):
        for d in range(1, peers):
            ag_copy(t, d, c).start()

    def norm(t, d):
        g = gain[0:1, :]
        b = bias[0:1, :]

        def one(i, carry):
            r = pl.ds(pl.multiple_of(i * NORM_ROWS, NORM_ROWS), NORM_ROWS)
            values = xs[t, d, r, :].astype(jnp.float32)
            centred = values - jnp.mean(values, axis=-1, keepdims=True)
            spread = jnp.mean(centred * centred, axis=-1, keepdims=True)
            h[r, :] = (centred * lax.rsqrt(spread + EPS) * g + b).astype(jnp.bfloat16)
            return carry

        lax.fori_loop(0, rows // NORM_ROWS, one, 0, unroll=2)

    def project(d, first):
        for i in range(n_tiles):
            if first:
                wi_copy(i).wait()
            cols = pl.ds(i * wi_tile, wi_tile)
            y = jnp.dot(h[...], wi[:, cols], preferred_element_type=jnp.float32)
            qkv[d * rows:(d + 1) * rows, cols] = y.astype(jnp.bfloat16)

    scale = math.log2(math.e) / math.sqrt(HD)

    def attend(t, d):
        r = slice(d * rows, (d + 1) * rows)
        for n in range(heads):
            base = n * 3 * HD
            q = qkv[r, base:base + HD]
            k = qkv[:, base + HD:base + 2 * HD]
            v = qkv[:, base + 2 * HD:base + 3 * HD]
            s = lax.dot_general(q, k, (((1,), (1,)), ((), ())), preferred_element_type=jnp.float32)
            e = jnp.exp2((s - jnp.max(s, axis=-1, keepdims=True)) * scale)
            total = jnp.sum(e, axis=-1, keepdims=True)
            y = jnp.dot(e.astype(jnp.bfloat16), v, preferred_element_type=jnp.float32)
            mixed[:, n * HD:(n + 1) * HD] = (y / total).astype(jnp.bfloat16)

        for c in range(n_chunks):
            y = jnp.dot(mixed[...], wo[:, span(c)], preferred_element_type=jnp.float32)
            part[t, d, :, span(c)] = y.astype(jnp.bfloat16)
            if d:
                rs_copy(t, d, c).start()

    def finish(t, c):
        for d in range(1, peers):
            rs_copy(t, d, c).wait_recv()

        def step(r):
            total = part[t, 0, r, span(c)].astype(jnp.float32)
            for d in range(1, peers):
                total = total + got[t, d - 1, r, span(c)].astype(jnp.float32)
            x = xs[t, 0, r, span(c)].astype(jnp.float32)
            res[t, r, span(c)] = (x + total).astype(jnp.bfloat16)

        pieces(step)

        @pl.when(has_next)
        def _():
            hop_copy(t, c).start()

    def take(t, c):
        chosen = order[0, t]

        @pl.when(has_prev)
        def _():
            hop_copy(t, c).wait_recv()

        def step(r, source):
            new = source[t, r, span(c)].astype(jnp.float32)
            for k in range(n_slots):
                old = slots[k, r, span(c)].astype(jnp.float32)
                slots[k, r, span(c)] = jnp.where(chosen == k, new, old).astype(jnp.bfloat16)

        @pl.when(has_prev)
        def _():
            pieces(functools.partial(step, source=arr))

        @pl.when(jnp.logical_not(has_prev))
        def _():
            pieces(functools.partial(step, source=fresh_v))

    def held_copy(c):
        return pltpu.make_async_copy(slots.at[:, :, span(c)], held.at[0, :, :, span(c)], held_sem.at[c])

    def out_copy(t):
        return pltpu.make_async_copy(res.at[t], out.at[t, 0], out_sem.at[t])

    for c in range(n_chunks):
        acts_copy(c).wait()
        offer(0, c)
    pl.semaphore_wait(
        barrier, peers - 1 + has_prev.astype(jnp.int32) + has_next.astype(jnp.int32)
    )
    for c in range(n_chunks):
        send_offer(0, c)

    for t in range(ticks):
        norm(t, 0)
        project(0, t == 0)
        for d in range(1, peers):
            for c in range(n_chunks):
                ag_copy(t, d, c).wait_recv()
            norm(t, d)
            project(d, False)
        if t == 0:
            load_wo.wait()
        for d in [*range(1, peers), 0]:
            attend(t, d)
        if t == 0:
            load_fresh.wait()
        lag = 1
        for step in range(n_chunks + lag):
            if step < n_chunks:
                finish(t, step)
            if step == n_chunks - 1:
                out_copy(t).start()
            if step >= lag:
                take(t, step - lag)
                if t + 1 < ticks:
                    offer(t + 1, step - lag)
                    send_offer(t + 1, step - lag)
                else:
                    held_copy(step - lag).start()

    for t in range(ticks):
        for c in range(n_chunks):
            for d in range(1, peers):
                ag_copy(t, d, c).wait_send()
                rs_copy(t, d, c).wait_send()

            @pl.when(has_next)
            def _():
                hop_copy(t, c).wait_send()

        out_copy(t).wait()
    for c in range(n_chunks):
        held_copy(c).wait()


def body(acts, fresh, order, ln_gain, ln_bias, wqkv, wo):
    ticks, rows, width = fresh.shape
    n_slots = acts.shape[1]
    peers = lax.axis_size("tensor")
    seq = rows * peers
    n_chunks = width // fitting(CHUNK, width)
    inner = wo.shape[1]
    wide = wqkv.shape[2]
    bf = jnp.bfloat16
    dma = pltpu.SemaphoreType.DMA
    anywhere = pl.BlockSpec(memory_space=pl.ANY)
    vmem = pl.BlockSpec(memory_space=pltpu.VMEM)
    smem = pl.BlockSpec(memory_space=pltpu.SMEM)
    return pl.pallas_call(
        relay,
        out_shape=(
            jax.ShapeDtypeStruct((ticks, 1, rows, width), bf),
            jax.ShapeDtypeStruct((1, n_slots, rows, width), bf),
        ),
        in_specs=[anywhere, anywhere, smem, vmem, vmem, anywhere, anywhere],
        out_specs=(anywhere, anywhere),
        scratch_shapes=[
            pltpu.VMEM((n_slots, rows, width), bf),
            pltpu.VMEM((ticks, rows, width), bf),
            pltpu.VMEM((width, wide), bf),
            pltpu.VMEM((inner, width), bf),
            pltpu.VMEM((ticks, peers, rows, width), bf),
            pltpu.VMEM((rows, width), bf),
            pltpu.VMEM((seq, wide), bf),
            pltpu.VMEM((rows, inner), bf),
            pltpu.VMEM((ticks, peers, rows, width), bf),
            pltpu.VMEM((ticks, peers - 1, rows, width), bf),
            pltpu.VMEM((ticks, rows, width), bf),
            pltpu.VMEM((ticks, rows, width), bf),
            dma((n_chunks,)),
            dma,
            dma((wide // fitting(TILE, wide),)),
            dma,
            dma((ticks,)),
            dma((n_chunks,)),
            dma((ticks, peers - 1, n_chunks)),
            dma((ticks, peers - 1, n_chunks)),
            dma((ticks, peers - 1, n_chunks)),
            dma((ticks, peers - 1, n_chunks)),
            dma((ticks, n_chunks)),
            dma((ticks, n_chunks)),
        ],
        compiler_params=pltpu.CompilerParams(
            collective_id=0, has_side_effects=True, vmem_limit_bytes=60 * 1024 * 1024
        ),
    )(acts, fresh, order, ln_gain, ln_bias, wqkv, wo)


def solution(mesh):
    return jax.shard_map(
        body,
        mesh=mesh,
        in_specs=(
            P("section", "dp", "tensor", None),
            P("dp", "tensor", None),
            P("section", None),
            P("section", None),
            P("section", None),
            P("section", None, "tensor"),
            P("section", "tensor", None),
        ),
        out_specs=(P("dp", "section", "tensor", None), P("section", "dp", "tensor", None)),
        check_vma=False,
    )
```

```python
import functools
import math

import jax
import jax.numpy as jnp
from jax import lax
from jax.experimental import pallas as pl
from jax.experimental.pallas import tpu as pltpu
from jax.sharding import PartitionSpec as P

HD = 128
EPS = 1e-06
CHUNK = 512
TILE = 1024
NORM_ROWS = 16
PIECE = 32
MESH = pl.DeviceIdType.MESH


def fitting(most, size):
    return math.gcd(most, size)


def relay(
    acts, fresh, order, gain, bias, w_in, w_out, out, held,
    slots, fresh_v, wi, wo, xs, h, qkv, mixed, part, got, res, arr,
    acts_sem, fresh_sem, wi_sem, wo_sem, out_sem, held_sem,
    ag_send, ag_recv, rs_send, rs_recv, hop_send, hop_recv,
):
    ticks, rows, width = fresh.shape
    n_slots = acts.shape[1]
    peers = lax.axis_size("tensor")
    sections = lax.axis_size("section")
    me = lax.axis_index("tensor")
    sec = lax.axis_index("section")
    seq = rows * peers
    heads = wi.shape[1] // (3 * HD)
    chunk = fitting(CHUNK, width)
    n_chunks = width // chunk
    wi_tile = fitting(TILE, wi.shape[1])
    n_tiles = wi.shape[1] // wi_tile
    has_prev = sec > 0
    has_next = sec < sections - 1

    def span(c):
        return pl.ds(c * chunk, chunk)

    def acts_copy(c):
        return pltpu.make_async_copy(acts.at[0, :, :, span(c)], slots.at[:, :, span(c)], acts_sem.at[c])

    for c in range(n_chunks):
        acts_copy(c).start()

    def wi_copy(i):
        cols = pl.ds(i * wi_tile, wi_tile)
        return pltpu.make_async_copy(w_in.at[0, :, cols], wi.at[:, cols], wi_sem.at[i])

    for i in range(n_tiles):
        wi_copy(i).start()
    load_wo = pltpu.make_async_copy(w_out.at[0], wo, wo_sem)
    load_wo.start()
    load_fresh = pltpu.make_async_copy(fresh, fresh_v, fresh_sem)
    load_fresh.start()

    barrier = pltpu.get_barrier_semaphore()
    for d in range(1, peers):
        pl.semaphore_signal(
            barrier, inc=1, device_id={"tensor": lax.rem(me + d, peers)}, device_id_type=MESH
        )

    @pl.when(has_prev)
    def _():
        pl.semaphore_signal(barrier, inc=1, device_id={"section": sec - 1}, device_id_type=MESH)

    @pl.when(has_next)
    def _():
        pl.semaphore_signal(barrier, inc=1, device_id={"section": sec + 1}, device_id_type=MESH)

    def ag_copy(t, d, c):
        return pltpu.make_async_remote_copy(
            src_ref=xs.at[t, 0, :, span(c)],
            dst_ref=xs.at[t, d, :, span(c)],
            send_sem=ag_send.at[t, d - 1, c],
            recv_sem=ag_recv.at[t, d - 1, c],
            device_id={"tensor": lax.rem(me + d, peers)},
            device_id_type=MESH,
        )

    def rs_copy(t, d, c):
        return pltpu.make_async_remote_copy(
            src_ref=part.at[t, d, :, span(c)],
            dst_ref=got.at[t, d - 1, :, span(c)],
            send_sem=rs_send.at[t, d - 1, c],
            recv_sem=rs_recv.at[t, d - 1, c],
            device_id={"tensor": lax.rem(me - d + peers, peers)},
            device_id_type=MESH,
        )

    def hop_copy(t, c):
        return pltpu.make_async_remote_copy(
            src_ref=res.at[t, :, span(c)],
            dst_ref=arr.at[t, :, span(c)],
            send_sem=hop_send.at[t, c],
            recv_sem=hop_recv.at[t, c],
            device_id={"section": lax.rem(sec + 1, sections)},
            device_id_type=MESH,
        )

    def pieces(step):
        for i in range(rows // PIECE):
            step(pl.ds(i * PIECE, PIECE))

    def offer(t, c):
        chosen = order[0, t]

        def step(r):
            x = slots[0, r, span(c)].astype(jnp.float32)
            for k in range(1, n_slots):
                x = jnp.where(chosen == k, slots[k, r, span(c)].astype(jnp.float32), x)
            xs[t, 0, r, span(c)] = x.astype(jnp.bfloat16)

        pieces(step)

    def send_offer(t, c):
        for d in range(1, peers):
            ag_copy(t, d, c).start()

    def norm(t, d):
        g = gain[0:1, :]
        b = bias[0:1, :]

        def one(i, carry):
            r = pl.ds(pl.multiple_of(i * NORM_ROWS, NORM_ROWS), NORM_ROWS)
            values = xs[t, d, r, :].astype(jnp.float32)
            centred = values - jnp.mean(values, axis=-1, keepdims=True)
            spread = jnp.mean(centred * centred, axis=-1, keepdims=True)
            h[r, :] = (centred * lax.rsqrt(spread + EPS) * g + b).astype(jnp.bfloat16)
            return carry

        lax.fori_loop(0, rows // NORM_ROWS, one, 0, unroll=2)

    def project(d, first):
        for i in range(n_tiles):
            if first:
                wi_copy(i).wait()
            cols = pl.ds(i * wi_tile, wi_tile)
            y = jnp.dot(h[...], wi[:, cols], preferred_element_type=jnp.float32)
            qkv[d * rows:(d + 1) * rows, cols] = y.astype(jnp.bfloat16)

    scale = math.log2(math.e) / math.sqrt(HD)

    def attend(t, d):
        r = slice(d * rows, (d + 1) * rows)
        for n in range(heads):
            base = n * 3 * HD
            q = qkv[r, base:base + HD]
            k = qkv[:, base + HD:base + 2 * HD]
            v = qkv[:, base + 2 * HD:base + 3 * HD]
            s = lax.dot_general(q, k, (((1,), (1,)), ((), ())), preferred_element_type=jnp.float32)
            e = jnp.exp2((s - jnp.max(s, axis=-1, keepdims=True)) * scale)
            total = jnp.sum(e, axis=-1, keepdims=True)
            y = jnp.dot(e.astype(jnp.bfloat16), v, preferred_element_type=jnp.float32)
            mixed[:, n * HD:(n + 1) * HD] = (y / total).astype(jnp.bfloat16)

        for c in range(n_chunks):
            y = jnp.dot(mixed[...], wo[:, span(c)], preferred_element_type=jnp.float32)
            part[t, d, :, span(c)] = y.astype(jnp.bfloat16)
            if d:
                rs_copy(t, d, c).start()

    def finish(t, c):
        for d in range(1, peers):
            rs_copy(t, d, c).wait_recv()

        def step(r):
            total = part[t, 0, r, span(c)].astype(jnp.float32)
            for d in range(1, peers):
                total = total + got[t, d - 1, r, span(c)].astype(jnp.float32)
            x = xs[t, 0, r, span(c)].astype(jnp.float32)
            res[t, r, span(c)] = (x + total).astype(jnp.bfloat16)

        pieces(step)

        @pl.when(has_next)
        def _():
            hop_copy(t, c).start()

    def take(t, c):
        chosen = order[0, t]

        @pl.when(has_prev)
        def _():
            hop_copy(t, c).wait_recv()

        def step(r, source):
            new = source[t, r, span(c)].astype(jnp.float32)
            for k in range(n_slots):
                old = slots[k, r, span(c)].astype(jnp.float32)
                slots[k, r, span(c)] = jnp.where(chosen == k, new, old).astype(jnp.bfloat16)

        @pl.when(has_prev)
        def _():
            pieces(functools.partial(step, source=arr))

        @pl.when(jnp.logical_not(has_prev))
        def _():
            pieces(functools.partial(step, source=fresh_v))

    def held_copy(c):
        return pltpu.make_async_copy(slots.at[:, :, span(c)], held.at[0, :, :, span(c)], held_sem.at[c])

    def out_copy(t):
        return pltpu.make_async_copy(res.at[t], out.at[t, 0], out_sem.at[t])

    for c in range(n_chunks):
        acts_copy(c).wait()
        offer(0, c)
    pl.semaphore_wait(
        barrier, peers - 1 + has_prev.astype(jnp.int32) + has_next.astype(jnp.int32)
    )
    for c in range(n_chunks):
        send_offer(0, c)

    for t in range(ticks):
        norm(t, 0)
        project(0, t == 0)
        for d in range(1, peers):
            for c in range(n_chunks):
                ag_copy(t, d, c).wait_recv()
            norm(t, d)
            project(d, False)
        if t == 0:
            load_wo.wait()
        for d in [*range(1, peers), 0]:
            attend(t, d)
        if t == 0:
            load_fresh.wait()
        lag = 1
        for step in range(n_chunks + lag):
            if step < n_chunks:
                finish(t, step)
            if step == n_chunks - 1:
                out_copy(t).start()
            if step >= lag:
                take(t, step - lag)
                if t + 1 < ticks:
                    offer(t + 1, step - lag)
                    send_offer(t + 1, step - lag)
                else:
                    held_copy(step - lag).start()

    for t in range(ticks):
        for c in range(n_chunks):
            for d in range(1, peers):
                ag_copy(t, d, c).wait_send()
                rs_copy(t, d, c).wait_send()

            @pl.when(has_next)
            def _():
                hop_copy(t, c).wait_send()

        out_copy(t).wait()
    for c in range(n_chunks):
        held_copy(c).wait()


def pin(*xs):
    return [pltpu.with_memory_space_constraint(x, pltpu.HBM) for x in xs]


def body(acts, fresh, order, ln_gain, ln_bias, wqkv, wo):
    ticks, rows, width = fresh.shape
    n_slots = acts.shape[1]
    peers = lax.axis_size("tensor")
    seq = rows * peers
    n_chunks = width // fitting(CHUNK, width)
    inner = wo.shape[1]
    wide = wqkv.shape[2]
    bf = jnp.bfloat16
    dma = pltpu.SemaphoreType.DMA
    anywhere = pl.BlockSpec(memory_space=pl.ANY)
    vmem = pl.BlockSpec(memory_space=pltpu.VMEM)
    smem = pl.BlockSpec(memory_space=pltpu.SMEM)
    return pl.pallas_call(
        relay,
        out_shape=(
            pltpu.VMEM((ticks, 1, rows, width), bf),
            pltpu.VMEM((1, n_slots, rows, width), bf),
        ),
        in_specs=[anywhere, anywhere, smem, vmem, vmem, anywhere, anywhere],
        out_specs=(vmem, vmem),
        scratch_shapes=[
            pltpu.VMEM((n_slots, rows, width), bf),
            pltpu.VMEM((ticks, rows, width), bf),
            pltpu.VMEM((width, wide), bf),
            pltpu.VMEM((inner, width), bf),
            pltpu.VMEM((ticks, peers, rows, width), bf),
            pltpu.VMEM((rows, width), bf),
            pltpu.VMEM((seq, wide), bf),
            pltpu.VMEM((rows, inner), bf),
            pltpu.VMEM((ticks, peers, rows, width), bf),
            pltpu.VMEM((ticks, peers - 1, rows, width), bf),
            pltpu.VMEM((ticks, rows, width), bf),
            pltpu.VMEM((ticks, rows, width), bf),
            dma((n_chunks,)),
            dma,
            dma((wide // fitting(TILE, wide),)),
            dma,
            dma((ticks,)),
            dma((n_chunks,)),
            dma((ticks, peers - 1, n_chunks)),
            dma((ticks, peers - 1, n_chunks)),
            dma((ticks, peers - 1, n_chunks)),
            dma((ticks, peers - 1, n_chunks)),
            dma((ticks, n_chunks)),
            dma((ticks, n_chunks)),
        ],
        compiler_params=pltpu.CompilerParams(
            collective_id=0, has_side_effects=True, vmem_limit_bytes=52 * 1024 * 1024
        ),
    )(*pin(acts, fresh), order, ln_gain, ln_bias, *pin(wqkv, wo))


def solution(mesh):
    return jax.shard_map(
        body,
        mesh=mesh,
        in_specs=(
            P("section", "dp", "tensor", None),
            P("dp", "tensor", None),
            P("section", None),
            P("section", None),
            P("section", None),
            P("section", None, "tensor"),
            P("section", "tensor", None),
        ),
        out_specs=(P("dp", "section", "tensor", None), P("section", "dp", "tensor", None)),
        check_vma=False,
    )
```

```python
import functools
import math

import jax
import jax.numpy as jnp
from jax import lax
from jax.experimental import pallas as pl
from jax.experimental.pallas import tpu as pltpu
from jax.sharding import PartitionSpec as P

HD = 128
EPS = 1e-06
CHUNK = 512
TILE = 1024
NORM_ROWS = 16
PIECE = 32
MESH = pl.DeviceIdType.MESH


def fitting(most, size):
    return math.gcd(most, size)


def relay(
    acts, fresh, order, gain, bias, w_in, w_out, out, held,
    slots, fresh_v, wi, wo, xs, h, hs, acc, qkv, mixed, part, got, arr,
    acts_sem, fresh_sem, wi_sem, wo_sem,
    ag_send, ag_recv, rs_send, rs_recv, hop_send, hop_recv,
):
    ticks, rows, width = fresh.shape
    n_slots = acts.shape[1]
    peers = lax.axis_size("tensor")
    sections = lax.axis_size("section")
    me = lax.axis_index("tensor")
    sec = lax.axis_index("section")
    seq = rows * peers
    heads = wi.shape[1] // (3 * HD)
    chunk = fitting(CHUNK, width)
    n_chunks = width // chunk
    wi_tile = fitting(TILE, wi.shape[1])
    n_tiles = wi.shape[1] // wi_tile
    has_prev = sec > 0
    has_next = sec < sections - 1

    def span(c):
        return pl.ds(c * chunk, chunk)

    def acts_copy(c):
        return pltpu.make_async_copy(acts.at[0, :, :, span(c)], slots.at[:, :, span(c)], acts_sem.at[c])

    for c in range(n_chunks):
        acts_copy(c).start()

    def wi_copy(i):
        cols = pl.ds(i * wi_tile, wi_tile)
        return pltpu.make_async_copy(w_in.at[0, :, cols], wi.at[:, cols], wi_sem.at[i])

    for i in range(n_tiles):
        wi_copy(i).start()
    load_wo = pltpu.make_async_copy(w_out.at[0], wo, wo_sem)
    load_wo.start()
    load_fresh = pltpu.make_async_copy(fresh, fresh_v, fresh_sem)
    load_fresh.start()

    barrier = pltpu.get_barrier_semaphore()
    for d in range(1, peers):
        pl.semaphore_signal(
            barrier, inc=1, device_id={"tensor": lax.rem(me + d, peers)}, device_id_type=MESH
        )

    @pl.when(has_prev)
    def _():
        pl.semaphore_signal(barrier, inc=1, device_id={"section": sec - 1}, device_id_type=MESH)

    @pl.when(has_next)
    def _():
        pl.semaphore_signal(barrier, inc=1, device_id={"section": sec + 1}, device_id_type=MESH)

    def ag_copy(t, d, c):
        src, dst = (xs.at[t, 0], xs.at[t, d]) if t else (hs.at[0], hs.at[d])
        return pltpu.make_async_remote_copy(
            src_ref=src.at[:, span(c)],
            dst_ref=dst.at[:, span(c)],
            send_sem=ag_send.at[t, d - 1, c],
            recv_sem=ag_recv.at[t, d - 1, c],
            device_id={"tensor": lax.rem(me + d, peers)},
            device_id_type=MESH,
        )

    def rs_copy(t, d, c):
        return pltpu.make_async_remote_copy(
            src_ref=part.at[t, d, :, span(c)],
            dst_ref=got.at[t, d - 1, :, span(c)],
            send_sem=rs_send.at[t, d - 1, c],
            recv_sem=rs_recv.at[t, d - 1, c],
            device_id={"tensor": lax.rem(me - d + peers, peers)},
            device_id_type=MESH,
        )

    def hop_copy(t, c):
        return pltpu.make_async_remote_copy(
            src_ref=out.at[t, 0, :, span(c)],
            dst_ref=arr.at[t, :, span(c)],
            send_sem=hop_send.at[t, c],
            recv_sem=hop_recv.at[t, c],
            device_id={"section": lax.rem(sec + 1, sections)},
            device_id_type=MESH,
        )

    def pieces(step):
        for i in range(rows // PIECE):
            step(pl.ds(i * PIECE, PIECE))

    def offer(t, c):
        chosen = order[0, t]

        def step(r):
            x = slots[0, r, span(c)].astype(jnp.float32)
            for k in range(1, n_slots):
                x = jnp.where(chosen == k, slots[k, r, span(c)].astype(jnp.float32), x)
            xs[t, 0, r, span(c)] = x.astype(jnp.bfloat16)

        pieces(step)

    def send_offer(t, c):
        for d in range(1, peers):
            ag_copy(t, d, c).start()

    def norm(t, d):
        into = h if t else hs.at[d]
        g = gain[0:1, :]
        b = bias[0:1, :]

        def one(i, carry):
            r = pl.ds(pl.multiple_of(i * NORM_ROWS, NORM_ROWS), NORM_ROWS)
            values = xs[t, d, r, :].astype(jnp.float32)
            centred = values - jnp.mean(values, axis=-1, keepdims=True)
            spread = jnp.mean(centred * centred, axis=-1, keepdims=True)
            into[r, :] = (centred * lax.rsqrt(spread + EPS) * g + b).astype(jnp.bfloat16)
            return carry

        lax.fori_loop(0, rows // NORM_ROWS, one, 0, unroll=2)

    def project(d, first):
        rows_in = hs.at[0] if first else h
        for i in range(n_tiles):
            if first:
                wi_copy(i).wait()
            cols = pl.ds(i * wi_tile, wi_tile)
            y = jnp.dot(rows_in[...], wi[:, cols], preferred_element_type=jnp.float32)
            qkv[d * rows:(d + 1) * rows, cols] = y.astype(jnp.bfloat16)

    def project_chunk(d, c):
        for i in range(n_tiles):
            cols = pl.ds(i * wi_tile, wi_tile)
            y = jnp.dot(
                hs[d, :, span(c)], wi[span(c), cols], preferred_element_type=jnp.float32
            )
            if c:
                y = acc[:, cols] + y
            if c + 1 < n_chunks:
                acc[:, cols] = y
            else:
                qkv[d * rows:(d + 1) * rows, cols] = y.astype(jnp.bfloat16)

    scale = math.log2(math.e) / math.sqrt(HD)

    def attend(t, d):
        r = slice(d * rows, (d + 1) * rows)
        for n in range(heads):
            base = n * 3 * HD
            q = qkv[r, base:base + HD]
            k = qkv[:, base + HD:base + 2 * HD]
            v = qkv[:, base + 2 * HD:base + 3 * HD]
            s = lax.dot_general(q, k, (((1,), (1,)), ((), ())), preferred_element_type=jnp.float32)
            e = jnp.exp2((s - jnp.max(s, axis=-1, keepdims=True)) * scale)
            total = jnp.sum(e, axis=-1, keepdims=True)
            y = jnp.dot(e.astype(jnp.bfloat16), v, preferred_element_type=jnp.float32)
            mixed[:, n * HD:(n + 1) * HD] = (y / total).astype(jnp.bfloat16)

        for c in range(n_chunks):
            y = jnp.dot(mixed[...], wo[:, span(c)], preferred_element_type=jnp.float32)
            part[t, d, :, span(c)] = y.astype(jnp.bfloat16)
            if d:
                rs_copy(t, d, c).start()

    def finish(t, c):
        for d in range(1, peers):
            rs_copy(t, d, c).wait_recv()

        def step(r):
            total = part[t, 0, r, span(c)].astype(jnp.float32)
            for d in range(1, peers):
                total = total + got[t, d - 1, r, span(c)].astype(jnp.float32)
            x = xs[t, 0, r, span(c)].astype(jnp.float32)
            out[t, 0, r, span(c)] = (x + total).astype(jnp.bfloat16)

        pieces(step)

        @pl.when(has_next)
        def _():
            hop_copy(t, c).start()

    def take(t, c):
        chosen = order[0, t]
        kept = slots if t + 1 < ticks else held.at[0]

        @pl.when(has_prev)
        def _():
            hop_copy(t, c).wait_recv()

        def step(r, source):
            new = source[t, r, span(c)].astype(jnp.float32)
            for k in range(n_slots):
                old = slots[k, r, span(c)].astype(jnp.float32)
                kept[k, r, span(c)] = jnp.where(chosen == k, new, old).astype(jnp.bfloat16)

        @pl.when(has_prev)
        def _():
            pieces(functools.partial(step, source=arr))

        @pl.when(jnp.logical_not(has_prev))
        def _():
            pieces(functools.partial(step, source=fresh_v))

    for c in range(n_chunks):
        acts_copy(c).wait()
        offer(0, c)
    norm(0, 0)
    pl.semaphore_wait(
        barrier, peers - 1 + has_prev.astype(jnp.int32) + has_next.astype(jnp.int32)
    )
    for c in range(n_chunks):
        send_offer(0, c)

    for t in range(ticks):
        if t:
            norm(t, 0)
        project(0, t == 0)
        for d in range(1, peers):
            for c in range(n_chunks):
                ag_copy(t, d, c).wait_recv()
                if t == 0:
                    project_chunk(d, c)
            if t:
                norm(t, d)
                project(d, False)
        if t == 0:
            load_wo.wait()
        for d in [*range(1, peers), 0]:
            attend(t, d)
        if t == 0:
            load_fresh.wait()
        lag = 1
        for step in range(n_chunks + lag):
            if step < n_chunks:
                finish(t, step)
            if step >= lag:
                take(t, step - lag)
                if t + 1 < ticks:
                    offer(t + 1, step - lag)
                    send_offer(t + 1, step - lag)

    for t in range(ticks):
        for c in range(n_chunks):
            for d in range(1, peers):
                ag_copy(t, d, c).wait_send()
                rs_copy(t, d, c).wait_send()

            @pl.when(has_next)
            def _():
                hop_copy(t, c).wait_send()


def pin(*xs):
    return [pltpu.with_memory_space_constraint(x, pltpu.HBM) for x in xs]


def body(acts, fresh, order, ln_gain, ln_bias, wqkv, wo):
    ticks, rows, width = fresh.shape
    n_slots = acts.shape[1]
    peers = lax.axis_size("tensor")
    seq = rows * peers
    n_chunks = width // fitting(CHUNK, width)
    inner = wo.shape[1]
    wide = wqkv.shape[2]
    bf = jnp.bfloat16
    dma = pltpu.SemaphoreType.DMA
    anywhere = pl.BlockSpec(memory_space=pl.ANY)
    vmem = pl.BlockSpec(memory_space=pltpu.VMEM)
    smem = pl.BlockSpec(memory_space=pltpu.SMEM)
    return pl.pallas_call(
        relay,
        out_shape=(
            pltpu.VMEM((ticks, 1, rows, width), bf),
            pltpu.VMEM((1, n_slots, rows, width), bf),
        ),
        in_specs=[anywhere, anywhere, smem, vmem, vmem, anywhere, anywhere],
        out_specs=(vmem, vmem),
        scratch_shapes=[
            pltpu.VMEM((n_slots, rows, width), bf),
            pltpu.VMEM((ticks, rows, width), bf),
            pltpu.VMEM((width, wide), bf),
            pltpu.VMEM((inner, width), bf),
            pltpu.VMEM((ticks, peers, rows, width), bf),
            pltpu.VMEM((rows, width), bf),
            pltpu.VMEM((peers, rows, width), bf),
            pltpu.VMEM((rows, wide), jnp.float32),
            pltpu.VMEM((seq, wide), bf),
            pltpu.VMEM((rows, inner), bf),
            pltpu.VMEM((ticks, peers, rows, width), bf),
            pltpu.VMEM((ticks, peers - 1, rows, width), bf),
            pltpu.VMEM((ticks, rows, width), bf),
            dma((n_chunks,)),
            dma,
            dma((wide // fitting(TILE, wide),)),
            dma,
            dma((ticks, peers - 1, n_chunks)),
            dma((ticks, peers - 1, n_chunks)),
            dma((ticks, peers - 1, n_chunks)),
            dma((ticks, peers - 1, n_chunks)),
            dma((ticks, n_chunks)),
            dma((ticks, n_chunks)),
        ],
        compiler_params=pltpu.CompilerParams(
            collective_id=0, has_side_effects=True, vmem_limit_bytes=52 * 1024 * 1024
        ),
    )(*pin(acts, fresh), order, ln_gain, ln_bias, *pin(wqkv, wo))


def solution(mesh):
    return jax.shard_map(
        body,
        mesh=mesh,
        in_specs=(
            P("section", "dp", "tensor", None),
            P("dp", "tensor", None),
            P("section", None),
            P("section", None),
            P("section", None),
            P("section", None, "tensor"),
            P("section", "tensor", None),
        ),
        out_specs=(P("dp", "section", "tensor", None), P("section", "dp", "tensor", None)),
        check_vma=False,
    )
```
